32 devices in a mesh: dp: 2 (over z, core), tp: 16 (over x, y).
Axes of the slice: x: 4, y: 4, z: 1, core: 2. Of those that a mesh axis runs over, the one named last changes fastest.
The devices are a block of a 4x4x8 slice.
Arguments:
- x: bfloat16 [4096, 14336], P('dp'), parts along dimension 0
- gain: bfloat16 [14336], replicated
- wq: bfloat16 [14336, 14336], P(None, 'tp')
- wk: bfloat16 [14336, 14336], P(None, 'tp')
- wv: bfloat16 [14336, 14336], P(None, 'tp')
- wo: bfloat16 [14336, 14336], P('tp')
Outputs:
- output: bfloat16 [4096, 14336], P('dp'), parts along dimension 0
There are 2 independent parts. The reference program is written for one: setup_inputs(seed, part) draws one part's arguments, and reference() takes and returns one part's arrays. A program takes and returns all parts, laid end to end along the dimension named above; an argument that names none is the same for every part.
All inputs are finite; a program needn't handle non-finite values.
Results may differ from the reference program's by a relative error of at most 0.012.
Values are sent between devices in bfloat16 or wider.
A program may use at most 768 MiB of HBM per device.

```python
import jax
import jax.numpy as jnp
from jax import lax

ROWS = 2048
D = 14336
HEADS = 112
KV_HEADS = 112
HEAD = 128
THETA = 10000


def setup_inputs(seed: int = 0, part: int = 0) -> dict:
    kx, kn, kq, kk, kv, ko = jax.random.split(jax.random.key(seed), 6)

    def weights(key, rows, columns):
        return jax.random.normal(key, (rows, columns), jnp.float32) * rows**-0.5

    drawn = {
        "x": jax.random.normal(jax.random.fold_in(kx, part), (ROWS, D), jnp.float32),
        "gain": 1 + 0.1 * jax.random.normal(kn, (D,), jnp.float32),
        "wq": 2 * weights(kq, D, HEADS * HEAD),
        "wk": 2 * weights(kk, D, KV_HEADS * HEAD),
        "wv": 4 * weights(kv, D, KV_HEADS * HEAD),
        "wo": weights(ko, HEADS * HEAD, D),
    }
    return {k: v.astype(jnp.bfloat16) for k, v in drawn.items()}


def normed(x, gain):
    wide = x.astype(jnp.float32)
    scale = lax.rsqrt(jnp.mean(wide * wide, -1, keepdims=True) + 1e-6)
    return (wide * scale * gain.astype(jnp.float32)).astype(jnp.bfloat16)


def turned(t, place, theta):
    half = t.shape[-1] // 2
    angle = place.astype(jnp.float32)[:, None] * theta ** (-jnp.arange(half, dtype=jnp.float32) / half)
    cos, sin = jnp.cos(angle)[:, None], jnp.sin(angle)[:, None]
    a, b = t[..., :half].astype(jnp.float32), t[..., half:].astype(jnp.float32)
    return jnp.concatenate([a * cos - b * sin, b * cos + a * sin], -1).astype(jnp.bfloat16)


def matmul(a, w):
    return jnp.dot(a, w, preferred_element_type=jnp.float32).astype(jnp.bfloat16)


def einsum(form, a, b):
    return jnp.einsum(form, a.astype(jnp.float32), b.astype(jnp.float32))


def attention(q, k, v):
    scores = einsum("tgsd,ugd->gstu", q, k) * q.shape[-1] ** -0.5
    token = jnp.arange(q.shape[0])
    scores = jnp.where(token[:, None] >= token, scores, -jnp.inf)
    weights = jax.nn.softmax(scores, -1).astype(jnp.bfloat16)
    return einsum("gstu,ugd->tgsd", weights, v).astype(jnp.bfloat16)


def reference(x, gain, wq, wk, wv, wo):
    a, place = normed(x, gain), jnp.arange(ROWS)
    q = turned(matmul(a, wq).reshape(ROWS, HEADS, HEAD), place, THETA).reshape(ROWS, KV_HEADS, -1, HEAD)
    k = turned(matmul(a, wk).reshape(ROWS, KV_HEADS, HEAD), place, THETA)
    v = matmul(a, wv).reshape(ROWS, KV_HEADS, HEAD)
    seen = attention(q, k, v).reshape(ROWS, HEADS * HEAD)
    return (x.astype(jnp.float32) + jnp.dot(seen, wo, preferred_element_type=jnp.float32)).astype(jnp.bfloat16)
```

```python
import functools
import math

import jax
import jax.numpy as jnp
from jax import lax
from jax.experimental import pallas as pl
from jax.experimental.pallas import tpu as pltpu
from jax.sharding import PartitionSpec as P

HEAD = 128
THETA = 10000
NEG = -1e30
HIDDEN = 2 * NEG
LOG2E = 1.4426950408889634
VMEM = 60 * 2**20
CUTS = (4, 4, 4, 4)
ANY = pl.BlockSpec(memory_space=pl.ANY)
MESH = pl.DeviceIdType.MESH


def _dot(a, b, ca=1, cb=0):
    return lax.dot_general(a, b, (((ca,), (cb,)), ((), ())), preferred_element_type=jnp.float32)


def _params(**kw):
    return pltpu.CompilerParams(vmem_limit_bytes=VMEM, **kw)


def _bf16(*shape):
    return jax.ShapeDtypeStruct(shape, jnp.bfloat16)


def _norm(x_ref, gain_ref, o_ref):
    wide = x_ref[...].astype(jnp.float32)
    scale = lax.rsqrt(jnp.mean(wide * wide, -1, keepdims=True) + 1e-6)
    o_ref[...] = (wide * scale * gain_ref[...].astype(jnp.float32)).astype(jnp.bfloat16)


def norm(x, gain, start, r):
    d = x.shape[1]
    b = 64
    return pl.pallas_call(
        _norm,
        grid=(r // b,),
        in_specs=[pl.BlockSpec((b, d), lambda i: (start // b + i, 0)), pl.BlockSpec((1, d), lambda i: (0, 0))],
        out_specs=pl.BlockSpec((b, d), lambda i: (i, 0)),
        out_shape=_bf16(r, d),
        compiler_params=_params(dimension_semantics=("arbitrary",)),
        cost_estimate=pl.CostEstimate(flops=r * d * 400, transcendentals=r, bytes_accessed=4 * r * d),
        name=f"norm_{start}",
    )(x, gain)


def _neighbours(side):
    t = lax.axis_index("tp")
    x, y = t // side, lax.rem(t, side)
    at = lambda i, j: {"tp": lax.rem(i, side) * side + lax.rem(j, side)}
    return x, y, at


def _greet(peers):
    barrier = pltpu.get_barrier_semaphore()
    for p in peers:
        pl.semaphore_signal(barrier, inc=1, device_id=p, device_id_type=MESH)
    pl.semaphore_wait(barrier, len(peers))


class Gather:
    def __init__(self, own, got, sems, side):
        x, y, at = _neighbours(side)
        self.peers = [at(x + 1, y), at(x + side - 1, y), at(x, y + 1), at(x, y + side - 1)]
        send, recv = sems
        h = own.shape[0] // 2

        def copy(src, dst, to, i):
            return pltpu.make_async_remote_copy(src, dst, send.at[i], recv.at[i], device_id=to, device_id_type=MESH)

        self.first, self.second = [], []
        for a in range(2):
            back, on, across = got[3 * a : 3 * a + 3]
            up, down = self.peers[2 * a : 2 * a + 2]
            self.first += [copy(own, back, up, 4 * a), copy(own, on, down, 4 * a + 1)]
            self.second += [
                copy(back.at[pl.ds(0, h)], across.at[pl.ds(0, h)], up, 4 * a + 2),
                copy(on.at[pl.ds(h, h)], across.at[pl.ds(h, h)], down, 4 * a + 3),
            ]

    def begin(self):
        _greet(self.peers)
        for c in self.first:
            c.start()

    def relay(self):
        for one, two in zip(self.first, self.second):
            one.wait_recv()
            two.start()

    def end(self):
        for c in self.second:
            c.wait_recv()
        for c in self.first + self.second:
            c.wait_send()


def _project(a_ref, wq_ref, wk_ref, wv_ref, *rest, deep, gather, side):
    if gather:
        own, rest = rest[0], rest[1:]
        got, rest = rest[3:9], rest[:3] + rest[9:]
        rest, sems = rest[:-2], rest[-2:]
        g = Gather(own, got, sems, side)
    outs, (w_s, acc, sem) = rest[:3], rest[3:]
    step, steps = pl.program_id(0), pl.num_programs(0)
    cols = wq_ref.shape[1]

    def copies(k, slot):
        rows = pl.ds(pl.multiple_of(k * deep, deep), deep)
        return [
            pltpu.make_async_copy(w.at[rows], w_s.at[slot, :, pl.ds(i * cols, cols)], sem.at[slot, i])
            for i, w in enumerate((wq_ref, wk_ref, wv_ref))
        ]

    @pl.when(step == 0)
    def _():
        for c in copies(0, 0):
            c.start()
        if gather:
            g.begin()

    @pl.when(step + 1 < steps)
    def _():
        for c in copies(step + 1, lax.rem(step + 1, 2)):
            c.start()

    if gather:
        pl.when(step == 4)(g.relay)

    slot = lax.rem(step, 2)
    for c in copies(step, slot):
        c.wait()
    got_ = _dot(a_ref[...], w_s[slot])

    @pl.when(step == 0)
    def _():
        acc[...] = got_

    @pl.when(step > 0)
    def _():
        acc[...] += got_

    @pl.when(step == steps - 1)
    def _():
        for i, o in enumerate(outs):
            o[...] = acc[:, i * cols : (i + 1) * cols].astype(jnp.bfloat16)
        if gather:
            g.end()


def project(a, wq, wk, wv, own, side, c):
    r, d = a.shape
    cols = wq.shape[1]
    deep = 2048
    gather = own is not None
    out = pl.BlockSpec((r, cols), lambda k: (0, 0))
    got = pl.pallas_call(
        functools.partial(_project, deep=deep, gather=gather, side=side),
        grid=(d // deep,),
        in_specs=[pl.BlockSpec((r, deep), lambda k: (0, k)), ANY, ANY, ANY] + [ANY] * gather,
        out_specs=[out] * 3 + [ANY] * (6 * gather),
        out_shape=[_bf16(r, cols)] * 3 + ([_bf16(*own.shape)] * 6 if gather else []),
        scratch_shapes=[
            pltpu.VMEM((2, deep, 3 * cols), jnp.bfloat16),
            pltpu.VMEM((r, 3 * cols), jnp.float32),
            pltpu.SemaphoreType.DMA((2, 3)),
        ]
        + ([pltpu.SemaphoreType.DMA((8,)), pltpu.SemaphoreType.DMA((8,))] if gather else []),
        compiler_params=_params(
            dimension_semantics=("arbitrary",), **(dict(collective_id=c, has_side_effects=True) if gather else {})
        ),
        cost_estimate=pl.CostEstimate(flops=6 * r * d * cols, transcendentals=0, bytes_accessed=6 * d * cols + 2 * r * d),
        name=f"project_{c}",
    )(a, wq, wk, wv, *([own] if gather else []))
    return got[:3], got[3:]


def _gather(own, *rest, side):
    g = Gather(own, rest[:6], rest[6:], side)
    g.begin()
    g.relay()
    g.end()


def gathered(own, side, c):
    return pl.pallas_call(
        functools.partial(_gather, side=side),
        in_specs=[ANY],
        out_specs=[ANY] * 6,
        out_shape=[_bf16(*own.shape)] * 6,
        scratch_shapes=[pltpu.SemaphoreType.DMA((8,)), pltpu.SemaphoreType.DMA((8,))],
        compiler_params=_params(collective_id=c, has_side_effects=True),
        cost_estimate=pl.CostEstimate(flops=own.size * 40000, transcendentals=0, bytes_accessed=8 * own.size),
        name=f"gather_{c}",
    )(own)


def _attention(q_ref, k_ref, v_ref, cos_ref, sin_ref, *rest, start, bk, last):
    o_ref, kc, vc = rest[2:5] if start else rest[:3]
    q_s, k_s, v_s, top_s, mix_s, sem = rest[-6:]
    r, cols = q_ref.shape
    d = HEAD
    heads = cols // d
    e = d**-0.5 * LOG2E
    before = []
    if start:
        before = [
            pltpu.make_async_copy(kc.at[pl.ds(0, start)], k_s.at[pl.ds(0, start)], sem.at[0]),
            pltpu.make_async_copy(vc.at[pl.ds(0, start)], v_s.at[pl.ds(0, start)], sem.at[1]),
        ]
        for c in before:
            c.start()
    cos, sin = cos_ref[...], sin_ref[...]
    for h in range(heads):
        at = slice(h * d, (h + 1) * d)
        for i, o, base in ((q_ref, q_s, 0), (k_ref, k_s, start)):
            t = i[:, at].astype(jnp.float32)
            o[base : base + r, at] = (t * cos + pltpu.roll(t, d // 2, 1) * sin).astype(jnp.bfloat16)
    v_s[start : start + r, :] = v_ref[...]
    top_s[...] = jnp.full(top_s.shape, NEG, jnp.float32)
    mix_s[...] = jnp.zeros(mix_s.shape, jnp.float32)
    ones = jnp.ones((8, bk), jnp.bfloat16)

    def block(j, masked):
        here = pl.ds(j * bk if isinstance(j, int) else pl.multiple_of(j * bk, bk), bk)
        scores = [_dot(k_s[here, h * d : (h + 1) * d], q_s[:, h * d : (h + 1) * d], 1, 1) for h in range(heads)]
        if masked:
            place = lax.broadcasted_iota(jnp.int32, (bk, r), 1) - lax.broadcasted_iota(jnp.int32, (bk, r), 0)
            ok = place >= j * bk - start
        weights, keeps = [], []
        for h, s in enumerate(scores):
            if masked:
                s = jnp.where(ok, s, HIDDEN)
            old = top_s[h : h + 1, :]
            top = jnp.maximum(old, s.max(axis=0, keepdims=True))
            top_s[h : h + 1, :] = top
            weights.append(jnp.exp2((s - top) * e).astype(jnp.bfloat16))
            keeps.append(jnp.exp2((old - top) * e))
        for h, (p, keep) in enumerate(zip(weights, keeps)):
            values = jnp.concatenate([v_s[here, h * d : (h + 1) * d].T, ones], axis=0)
            mix_s[h] = mix_s[h] * keep + _dot(values, p)

    for j in range(start // bk, (start + r) // bk):
        block(j, True)
    for c in before:
        c.wait()
    if start:
        lax.fori_loop(0, start // bk, lambda j, _: block(j, False), None)
    after = []
    if not last:
        after = [
            pltpu.make_async_copy(k_s.at[pl.ds(start, r)], kc.at[pl.ds(start, r)], sem.at[2]),
            pltpu.make_async_copy(v_s.at[pl.ds(start, r)], vc.at[pl.ds(start, r)], sem.at[3]),
        ]
        for c in after:
            c.start()
    for h in range(heads):
        o_ref[:, h * d : (h + 1) * d] = (mix_s[h, :d, :] * (1 / mix_s[h, d : d + 1, :])).T.astype(o_ref.dtype)
    for c in after:
        c.wait()


def attention(qkv, cos, sin, caches, start, rows):
    r, cols = qkv[0].shape
    heads = cols // HEAD
    seen = start + r
    bk = 256 if r % 512 else 512
    bk = bk if start % bk == 0 else 128
    unit = math.gcd(start, r) if start else r
    chunk = pl.BlockSpec((r, cols), lambda i: (0, 0))
    cache = _bf16(rows, cols)
    whole = pl.BlockSpec((r, HEAD), lambda i: (0, 0))
    return pl.pallas_call(
        functools.partial(_attention, start=start, bk=bk, last=seen == rows),
        grid=(1,),
        in_specs=[chunk] * 3 + [whole] * 2 + [ANY] * (2 if start else 0),
        out_specs=[chunk, ANY, ANY],
        out_shape=[_bf16(r, cols), cache, cache],
        input_output_aliases={5: 1, 6: 2} if start else {},
        scratch_shapes=[
            pltpu.VMEM((r, cols), jnp.bfloat16),
            pltpu.VMEM((seen, cols), jnp.bfloat16),
            pltpu.VMEM((seen, cols), jnp.bfloat16),
            pltpu.VMEM((heads, r), jnp.float32),
            pltpu.VMEM((heads, HEAD + 8, r), jnp.float32),
            pltpu.SemaphoreType.DMA((4,)),
        ],
        compiler_params=_params(dimension_semantics=("arbitrary",)),
        cost_estimate=pl.CostEstimate(flops=8 * heads * r * seen * HEAD, transcendentals=heads * r * seen,
                                      bytes_accessed=2 * cols * (2 * seen + 4 * r)),
        name=f"attention_{start}",
    )(*qkv, cos[start : start + r], sin[start : start + r], *(caches if start else ()))


def _finish(x_ref, wo_ref, own_ref, *rest, side, start):
    n = side - 1
    got, rest = (rest[:n], rest[n : 2 * n]), rest[2 * n :]
    cut = [(rest[2 * n * a : 2 * n * a + n], rest[2 * n * a + n : 2 * n * a + 2 * n]) for a in range(2)]
    o_ref = rest[4 * n]
    s_s, w_s, total, keep_s, send_s, recv_s, res_s, s_sem, w_sem, r_sem, send_sem, recv_sem = rest[4 * n + 1 :]
    x, y, at = _neighbours(side)
    core = lax.rem(lax.axis_index("dp"), 2)
    r, deep = own_ref.shape
    rows, quarter = o_ref.shape[1:]
    half = quarter // 2
    place = (y, x)
    col0 = (x * quarter, (side + y) * quarter)
    peers = ([at(x, y + k) for k in range(1, side)], [at(x + k, y) for k in range(1, side)])

    def seen_copies(a):
        return [pltpu.make_async_copy(s, s_s.at[a, :, pl.ds(j * deep, deep)], s_sem.at[a, j]) for j, s in enumerate((own_ref, *got[a]))]

    tiles = [(0, 0), (1, 0), (0, 1), (1, 1)]

    def w_copies(i):
        a, b = tiles[i]
        first = pl.multiple_of(col0[a] + lax.rem(core + b, 2) * half, 128)
        slot = i % 2
        return [
            pltpu.make_async_copy(w, w_s.at[slot, pl.ds(j * deep, deep), :], w_sem.at[slot, j])
            for j, w in enumerate((wo_ref.at[:, pl.ds(first, half)], *cut[a][b]))
        ]

    res = [
        pltpu.make_async_copy(
            x_ref.at[pl.ds(pl.multiple_of(start + place[a] * rows, rows), rows), pl.ds(pl.multiple_of(col0[a], 128), quarter)],
            res_s.at[a], r_sem.at[a],
        )
        for a in range(2)
    ]
    seen = [seen_copies(0), seen_copies(1)]
    for c in seen[0] + w_copies(0) + seen[1] + res:
        c.start()
    _greet(peers[0] + peers[1])
    sent = []
    for i, (a, b) in enumerate(tiles):
        if i + 1 < len(tiles):
            for c in w_copies(i + 1):
                c.start()
        if b == 0:
            for c in seen[a]:
                c.wait()
        for c in w_copies(i):
            c.wait()
        total[...] = _dot(s_s[a], w_s[i % 2])
        to = pl.ds(pl.multiple_of(lax.rem(core + b, 2) * half, 128), half)
        piece = lambda k: total[pl.ds(pl.multiple_of(lax.rem(place[a] + k, side) * rows, rows), rows), :]
        for k in (2, 1, 3):
            send_s[a, b, k - 1] = piece(k).astype(jnp.bfloat16)
            c = pltpu.make_async_remote_copy(
                send_s.at[a, b, k - 1], recv_s.at[a, b, k - 1], send_sem.at[a, b, k - 1], recv_sem.at[a, b, k - 1],
                device_id=peers[a][k - 1], device_id_type=MESH,
            )
            c.start()
            sent.append(c)
        keep_s[a, b] = piece(0)
    for c in res:
        c.wait()
    for i, (a, b) in enumerate(tiles):
        to = pl.ds(pl.multiple_of(lax.rem(core + b, 2) * half, 128), half)
        for k in range(3):
            sent[3 * i + k].wait_recv()
        total_ = keep_s[a, b] + sum(recv_s[a, b, k].astype(jnp.float32) for k in range(n))
        o_ref[a, :, to] = (res_s[a, :, to].astype(jnp.float32) + total_).astype(jnp.bfloat16)
    for c in sent:
        c.wait_send()


def finish(x, wo, own, got, cut, side, start, c):
    r, deep = own.shape
    d = x.shape[1]
    quarter = d // 2 // side
    half = quarter // 2
    rows = r // side
    n = side - 1
    dma = pltpu.SemaphoreType.DMA
    return pl.pallas_call(
        functools.partial(_finish, side=side, start=start),
        in_specs=[ANY] * (3 + 2 * n + 4 * n),
        out_specs=pl.BlockSpec(memory_space=pltpu.VMEM),
        out_shape=_bf16(2, rows, quarter),
        scratch_shapes=[
            pltpu.VMEM((2, r, side * deep), jnp.bfloat16),
            pltpu.VMEM((2, side * deep, half), jnp.bfloat16),
            pltpu.VMEM((r, half), jnp.float32),
            pltpu.VMEM((2, 2, rows, half), jnp.float32),
            pltpu.VMEM((2, 2, n, rows, half), jnp.bfloat16),
            pltpu.VMEM((2, 2, n, rows, half), jnp.bfloat16),
            pltpu.VMEM((2, rows, quarter), jnp.bfloat16),
            dma((2, side)), dma((2, side)), dma((2,)), dma((2, 2, n)), dma((2, 2, n)),
        ],
        compiler_params=_params(collective_id=c, has_side_effects=True),
        cost_estimate=pl.CostEstimate(flops=4 * r * deep * d, transcendentals=0, bytes_accessed=2 * deep * d),
        name=f"finish_{c}",
    )(x, wo, own, *got, *cut[0][0], *cut[0][1], *cut[1][0], *cut[1][1])


def _lay(got_ref, *rest, side, start):
    y_ref, buf, in_sem, out_sem = rest[-4:]
    n, _, rows, quarter = got_ref.shape

    def spot(t, a):
        i, j = t // side, t % side
        i, j = (j, i) if a == 0 else (i, side + j)
        return y_ref.at[pl.ds(start + i * rows, rows), pl.ds(j * quarter, quarter)]

    ins = [pltpu.make_async_copy(got_ref.at[t], buf.at[t], in_sem.at[t]) for t in range(n)]
    outs = [pltpu.make_async_copy(buf.at[t, a], spot(t, a), out_sem.at[t, a]) for t in range(n) for a in range(2)]
    for c in ins:
        c.start()
    for t in range(n):
        ins[t].wait()
        outs[2 * t].start()
        outs[2 * t + 1].start()
    for c in outs:
        c.wait()


def lay(got, y, shape, start, side):
    first = y is None
    n = got.shape[0]
    return pl.pallas_call(
        functools.partial(_lay, side=side, start=start),
        in_specs=[ANY] * (1 if first else 2),
        out_specs=ANY,
        out_shape=_bf16(*shape),
        scratch_shapes=[pltpu.VMEM(got.shape, jnp.bfloat16), pltpu.SemaphoreType.DMA((n,)), pltpu.SemaphoreType.DMA((n, 2))],
        input_output_aliases={} if first else {1: 0},
        compiler_params=_params(),
        cost_estimate=pl.CostEstimate(flops=400 * got.size, transcendentals=0, bytes_accessed=4 * got.size),
        name=f"lay_{start}",
    )(got, *(() if first else (y,)))


def solution(mesh):
    side = math.isqrt(mesh.shape["tp"])
    pairs = [(i, i ^ 1) for i in range(mesh.shape["dp"])]

    def along(a, s):
        moved = lambda i, j: ((i + s) % side, j) if a == 0 else (i, (j + s) % side)
        return [(i * side + j, u * side + v) for i in range(side) for j in range(side) for u, v in [moved(i, j)]]

    def step(x, gain, wq, wk, wv, wo):
        rows, d = x.shape
        sizes = [rows * c // sum(CUTS) for c in CUTS]
        starts = [sum(sizes[:i]) for i in range(len(sizes))]
        t = lax.axis_index("tp")
        place, core = (t // side, t % side), lax.axis_index("dp") % 2
        quarter = d // 2 // side
        half = quarter // 2

        order = (1, side - 1, 2)
        mine = [
            [
                lax.ppermute(
                    lax.dynamic_slice_in_dim(wo, (a * side + (place[a] + s) % side) * quarter + core * half, half, 1), "tp", along(a, s)
                )
                for s in order
            ]
            for a in range(2)
        ]
        cut = [(m, [lax.ppermute(w, "dp", pairs) for w in m]) for m in mine]

        angle = jnp.arange(rows, dtype=jnp.float32)[:, None] * THETA ** (-jnp.arange(HEAD // 2, dtype=jnp.float32) / (HEAD // 2))
        cos, sin = jnp.cos(angle), jnp.sin(angle)
        cos, sin = jnp.concatenate([cos, cos], 1), jnp.concatenate([-sin, sin], 1)

        caches, y, own, blocks = None, None, None, []

        def end(i, own, got):
            block = finish(x, wo, own, got, cut, side, starts[i], len(sizes) + i)
            blocks.append(lax.all_gather(block, "tp"))

        for i, (start, r) in enumerate(zip(starts, sizes)):
            qkv, got = project(norm(x, gain[None], start, r), wq, wk, wv, own, side, i)
            if i:
                end(i - 1, own, got)
            own, *caches = attention(qkv, cos, sin, caches, start, rows)
        end(len(sizes) - 1, own, gathered(own, side, 2 * len(sizes)))
        for start, got in zip(starts, blocks):
            y = lay(got, y, x.shape, start, side)
        return y

    tokens, columns = P("dp", None), P(None, "tp")
    return jax.shard_map(
        step,
        mesh=mesh,
        in_specs=(tokens, P(None), columns, columns, columns, P("tp", None)),
        out_specs=tokens,
        check_vma=False,
    )
```

```python
import functools
import math

import jax
import jax.numpy as jnp
from jax import lax
from jax.experimental import pallas as pl
from jax.experimental.pallas import tpu as pltpu
from jax.sharding import PartitionSpec as P

HEAD = 128
THETA = 10000
NEG = -1e30
HIDDEN = 2 * NEG
LOG2E = 1.4426950408889634
VMEM = 63 * 2**20
CHUNK = 256
PIECE = 64
DEEP = 1024
SLOTS = 3
ANY = pl.BlockSpec(memory_space=pl.ANY)
MESH = pl.DeviceIdType.MESH


def _dot(a, b, ca=1, cb=0):
    return lax.dot_general(a, b, (((ca,), (cb,)), ((), ())), preferred_element_type=jnp.float32)


def _params(**kw):
    return pltpu.CompilerParams(vmem_limit_bytes=VMEM, **kw)


def _bf16(*shape):
    return jax.ShapeDtypeStruct(shape, jnp.bfloat16)


def _times(n, size):
    return pl.ds(pl.multiple_of(n * size, size), size)


class Copies:
    def __init__(self, *copies):
        self.copies = copies

    def start(self):
        for c in self.copies:
            c.start()

    def arrive(self):
        for c in self.copies:
            c.wait_recv()

    def leave(self):
        for c in self.copies:
            c.wait_send()


def _layer(x_ref, gain_ref, wq_ref, wk_ref, wv_ref, wo_ref, cos_ref, sin_ref, g0_ref, g1_ref, last_ref, cut_ref,
           xin, a_s, w_s, acc, q_s, k_s, v_s, top_s, mix_s, s_s, keep_s, send_s, recv_s, res_s, blk_s,
           x_sem, w_sem, res_sem, blk_sem, cut_send, cut_recv, swap_send, swap_recv,
           ring_send, ring_recv, sum_send, sum_recv, all_send, all_recv, *, side):
    total_rows, d = x_ref.shape
    cols = wq_ref.shape[1]
    r, n = CHUNK, total_rows // CHUNK
    heads = cols // HEAD
    quarter = d // 2 // side
    half = quarter // 2
    rows = r // side
    steps = d // DEEP
    tiles = 2 * side
    per = steps + tiles
    t, dp = lax.axis_index("tp"), lax.axis_index("dp")
    x, y = lax.div(t, side), lax.rem(t, side)
    core = lax.rem(dp, 2)
    g_ref = (g0_ref, g1_ref)

    def at(i, j):
        return {"tp": lax.rem(i, side) * side + lax.rem(j, side)}

    def along(a, k):
        return at(x + (1 - a) * k, y + a * k)

    own_place = lambda a: x + a * (y - x)
    sum_place = lambda a: own_place(1 - a)
    col0 = lambda a: pl.multiple_of((a * side + own_place(a)) * quarter, 128)
    sibling = {"dp": dp + 1 - 2 * core}

    def remote(src, dst, send, recv, to):
        return pltpu.make_async_remote_copy(src, dst, send, recv, device_id=to, device_id_type=MESH)

    place_of = {1: 0, side - 1: 1, 2: 2}

    def cut(ks):
        out = []
        for a in range(2):
            for k in ks:
                i = place_of[k]
                first = (a * side + lax.rem(own_place(a) + k, side)) * quarter + core * half
                out.append(remote(wo_ref.at[:, pl.ds(pl.multiple_of(first, 128), half)], cut_ref.at[a, 0, i],
                                  cut_send.at[a, i], cut_recv.at[a, i], along(a, k)))
        return Copies(*out)

    def swap(places):
        return Copies(*[
            remote(cut_ref.at[a, 0, i], cut_ref.at[a, 1, i], swap_send.at[a, i], swap_recv.at[a, i], sibling)
            for a in range(2) for i in places
        ])

    near, far = cut((1, side - 1)), cut((2,))
    near_swap, far_swap = swap((0, 1)), swap((2,))

    def ring(c):
        slot = lax.rem(c, 2)
        h = r // 2
        first, second = [], []
        for a in range(2):
            up, down = along(a, 1), along(a, side - 1)
            own, back, on, across = (s_s.at[slot, a, j] for j in range(4))
            pair = lambda src, dst, i, to: remote(src, dst, ring_send.at[slot, a, i], ring_recv.at[slot, a, i], to)
            first += [pair(own, back, 0, up), pair(own, on, 1, down)]
            second += [
                pair(back.at[pl.ds(0, h)], across.at[pl.ds(0, h)], 2, up),
                pair(on.at[pl.ds(h, h)], across.at[pl.ds(h, h)], 3, down),
            ]
        return Copies(*first), Copies(*second)

    def everywhere(c):
        slot = lax.rem(c, 2)
        h, m = rows // 2, side // 2
        one, two, three, four = [], [], [], []
        for a in range(2):
            g = g_ref[a].at[c]
            i, j = own_place(1 - a), own_place(a)
            pair = lambda ref, k, to: remote(ref, ref, all_send.at[slot, a, k], all_recv.at[slot, a, k], to)
            up, down = along(a, 1), along(a, side - 1)
            one += [pair(g.at[i, j], 0, up), pair(g.at[i, j], 1, down)]
            back, on = lax.rem(j + side - 1, side), lax.rem(j + 1, side)
            two += [pair(g.at[i, back, pl.ds(0, h)], 2, up), pair(g.at[i, on, pl.ds(h, h)], 3, down)]
            up, down = along(1 - a, 1), along(1 - a, side - 1)
            three += [pair(g.at[i], 4, up), pair(g.at[i], 5, down)]
            back, on = lax.rem(i + side - 1, side), lax.rem(i + 1, side)
            four += [pair(g.at[back, pl.ds(0, m)], 6, up), pair(g.at[on, pl.ds(m, m)], 7, down)]
        return Copies(*one), Copies(*two), Copies(*three), Copies(*four)

    def x_copy(c, i):
        slot = lax.rem(i, 2)
        return pltpu.make_async_copy(x_ref.at[pl.ds(pl.multiple_of(c * r + i * PIECE, PIECE), PIECE)], xin.at[slot], x_sem.at[slot])

    def w_slot(p, i):
        return lax.rem(p * per + i, SLOTS)

    def w_copies(p, i):
        slot = w_slot(p, i)
        return [
            pltpu.make_async_copy(w.at[_times(i, DEEP)], w_s.at[slot, :, pl.ds(k * cols, cols)], w_sem.at[slot, k])
            for k, w in enumerate((wq_ref, wk_ref, wv_ref))
        ]

    def o_copies(p, u):
        slot = w_slot(p, steps + u)
        a, j = lax.div(u, side), lax.rem(u, side)
        here = w_s.at[slot, pl.ds(0, cols)]
        own = pltpu.make_async_copy(wo_ref.at[:, pl.ds(col0(a), quarter)], here.at[:, pl.ds(0, quarter)], w_sem.at[slot, 0])
        i = jnp.maximum(j - 1, 0)
        others = [
            pltpu.make_async_copy(cut_ref.at[a, b, i],
                                  here.at[:, pl.ds(pl.multiple_of(lax.rem(core + b, 2) * half, 128), half)], w_sem.at[slot, 1 + b])
            for b in range(2)
        ]
        return j, own, others

    def o_start(p, u):
        j, own, others = o_copies(p, u)
        pl.when(j == 0)(own.start)

        @pl.when(j > 0)
        def _():
            for c in others:
                c.start()

    def o_wait(p, u):
        j, own, others = o_copies(p, u)
        pl.when(j == 0)(own.wait)

        @pl.when(j > 0)
        def _():
            for c in others:
                c.wait()

    def w_start(p, i):
        for c in w_copies(p, i):
            c.start()

    def sums(c, a):
        slot = lax.rem(c, 2)
        return Copies(*[
            remote(send_s.at[a, k - 1], recv_s.at[slot, a, k - 1], sum_send.at[slot, a, k - 1], sum_recv.at[slot, a, k - 1], along(1 - a, k))
            for k in (2, 1, 3)
        ])

    def residual(c):
        return [
            pltpu.make_async_copy(
                x_ref.at[pl.ds(pl.multiple_of(c * r + sum_place(a) * rows, rows), rows), pl.ds(col0(a), quarter)], res_s.at[a], res_sem.at[a]
            )
            for a in range(2)
        ]

    def block_copies(c):
        return [pltpu.make_async_copy(blk_s.at[a], g_ref[a].at[c, own_place(1 - a), own_place(a)], blk_sem.at[a]) for a in range(2)]

    def norm(p):
        def piece(i, _):
            x_copy(p, i).wait()
            wide = xin[lax.rem(i, 2)].astype(jnp.float32)
            scale = lax.rsqrt(jnp.mean(wide * wide, -1, keepdims=True) + 1e-6)
            a_s[_times(i, PIECE), :] = (wide * scale * gain_ref[...].astype(jnp.float32)).astype(jnp.bfloat16)

            @pl.when(i + 2 < r // PIECE)
            def _():
                x_copy(p, i + 2).start()

        lax.fori_loop(0, r // PIECE, piece, None)

    def project(p, hooks):
        def at_step(i, _):
            @pl.when(i + 2 < steps)
            def _():
                w_start(p, i + 2)

            @pl.when((i + 2 >= steps) & (p > 0))
            def _():
                o_start(p, i + 2 - steps)

            hooks(i)
            for c in w_copies(p, i):
                c.wait()
            got = _dot(a_s[:, _times(i, DEEP)], w_s[w_slot(p, i)])

            @pl.when(i == 0)
            def _():
                acc[...] = got

            @pl.when(i > 0)
            def _():
                acc[...] += got

        lax.fori_loop(0, steps, at_step, None)
        here = _times(p, r)
        cos, sin = cos_ref[here, :], sin_ref[here, :]
        turn = lambda t: (t * cos + pltpu.roll(t, HEAD // 2, 1) * sin).astype(jnp.bfloat16)
        for h in range(heads):
            a = slice(h * HEAD, (h + 1) * HEAD)
            q_s[:, a] = turn(acc[:, a].astype(jnp.bfloat16).astype(jnp.float32))
            k_s[here, a] = turn(acc[:, cols + h * HEAD : cols + (h + 1) * HEAD].astype(jnp.bfloat16).astype(jnp.float32))
        v_s[here, :] = acc[:, 2 * cols :].astype(jnp.bfloat16)

    def attend(p):
        e = HEAD**-0.5 * LOG2E
        top_s[...] = jnp.full(top_s.shape, NEG, jnp.float32)
        mix_s[...] = jnp.zeros(mix_s.shape, jnp.float32)
        ones = jnp.ones((8, r), jnp.bfloat16)

        def block(j, masked):
            here = _times(j, r)
            scores = [_dot(k_s[here, h * HEAD : (h + 1) * HEAD], q_s[:, h * HEAD : (h + 1) * HEAD], 1, 1) for h in range(heads)]
            if masked:
                ok = lax.broadcasted_iota(jnp.int32, (r, r), 1) >= lax.broadcasted_iota(jnp.int32, (r, r), 0)
            weights, keeps = [], []
            for h, s in enumerate(scores):
                if masked:
                    s = jnp.where(ok, s, HIDDEN)
                old = top_s[h : h + 1, :]
                top = jnp.maximum(old, s.max(axis=0, keepdims=True))
                top_s[h : h + 1, :] = top
                weights.append(jnp.exp2((s - top) * e).astype(jnp.bfloat16))
                keeps.append(jnp.exp2((old - top) * e))
            for h, (w, keep) in enumerate(zip(weights, keeps)):
                values = jnp.concatenate([v_s[here, h * HEAD : (h + 1) * HEAD].T, ones], axis=0)
                mix_s[h] = mix_s[h] * keep + _dot(values, w)

        lax.fori_loop(0, p, lambda j, _: block(j, False), None)
        block(p, True)
        slot = lax.rem(p, 2)
        for h in range(heads):
            got = (mix_s[h, :HEAD, :] * (1 / mix_s[h, HEAD : HEAD + 1, :])).T.astype(jnp.bfloat16)
            for a in range(2):
                s_s[slot, a, 0, :, h * HEAD : (h + 1) * HEAD] = got

    def output(p, c):
        slot = lax.rem(c, 2)

        def tile(u, _):
            @pl.when(u + 2 < tiles)
            def _():
                o_start(p, u + 2)

            @pl.when((u + 2 >= tiles) & (p + 1 < n))
            def _():
                w_start(p + 1, u + 2 - tiles)

            pl.when((p == 1) & (u == 0))(far_swap.arrive)
            a, j = lax.div(u, side), lax.rem(u, side)
            o_wait(p, u)
            got = _dot(s_s[slot, a, j], w_s[w_slot(p, steps + u), :cols, :quarter])

            @pl.when(j == 0)
            def _():
                acc[:, :quarter] = got

            @pl.when(j > 0)
            def _():
                acc[:, :quarter] += got

            @pl.when(j == side - 1)
            def _():
                part = lambda k: acc[_times(lax.rem(sum_place(a) + k, side), rows), :quarter]
                for k in (2, 1, 3):
                    send_s[a, k - 1] = part(k).astype(jnp.bfloat16)
                keep_s[a] = part(0)
                sums(c, a).start()

        lax.fori_loop(0, tiles, tile, None)

    def finish(c):
        slot = lax.rem(c, 2)
        for c_ in residual(c):
            c_.wait()
        for a in range(2):
            s = sums(c, a)
            s.arrive()
            total = keep_s[a] + sum(recv_s[slot, a, k].astype(jnp.float32) for k in range(side - 1))
            blk_s[a] = (res_s[a].astype(jnp.float32) + total).astype(jnp.bfloat16)
            s.leave()

    for i in range(2):
        x_copy(0, i).start()
        w_start(0, i)
    peers = [along(a, k) for a in range(2) for k in range(1, side)] + [sibling]
    barrier = pltpu.get_barrier_semaphore()
    for p in peers:
        pl.semaphore_signal(barrier, inc=1, device_id=p, device_id_type=MESH)
    pl.semaphore_wait(barrier, len(peers))
    near.start()
    far.start()

    def period(p, _):
        some, c = p > 0, p - 1

        @pl.when(some)
        def _():
            ring(c)[0].start()
            for k in residual(c):
                k.start()

        @pl.when(p > 1)
        def _():
            for k in block_copies(p - 2):
                k.wait()
            everywhere(p - 2)[0].start()

        def relay_ring():
            first, second = ring(c)
            first.arrive()
            second.start()

        def relay_one():
            one, two, _, _ = everywhere(p - 2)
            one.arrive()
            two.start()

        def begin_three():
            _, two, three, _ = everywhere(p - 2)
            two.arrive()
            three.start()

        def end_all(c):
            four = everywhere(c)
            four[3].arrive()
            for k in four:
                k.leave()

        def hooks(i):
            pl.when((p > 1) & (i == A1))(relay_ring)
            pl.when((p > 2) & (i == A1))(lambda: end_all(p - 3))
            pl.when((p > 1) & (i == B1))(relay_one)
            pl.when((p > 1) & (i == B2))(begin_three)

            @pl.when((p == 1) & (i == steps - 3))
            def _():
                near_swap.arrive()
                far.arrive()
                far_swap.start()

            pl.when((p == 1) & (i == steps - 1))(relay_ring)

        @pl.when(p < n)
        def _():
            norm(p)

            @pl.when(p + 1 < n)
            def _():
                for i in range(2):
                    x_copy(p + 1, i).start()

            project(p, hooks)

        @pl.when(p == 0)
        def _():
            near.arrive()
            near_swap.start()
            for i in range(2):
                w_start(1, i)

        @pl.when(p == n)
        def _():
            for u in range(2):
                o_start(p, u)
            relay_ring()
            end_all(p - 3)
            relay_one()
            begin_three()

        @pl.when(some)
        def _():
            first, second = ring(c)
            second.arrive()
            output(p, c)
            first.leave()
            second.leave()

        @pl.when(p > 1)
        def _():
            _, _, three, four = everywhere(p - 2)
            three.arrive()
            four.start()

        @pl.when(p < n)
        def _():
            attend(p)

        @pl.when(some)
        def _():
            finish(c)

        @pl.when(some & (p < n))
        def _():
            for k in block_copies(c):
                k.start()

    lax.fori_loop(0, n + 1, period, None)
    out = pltpu.make_async_copy(blk_s, last_ref, blk_sem.at[0])
    out.start()
    four = everywhere(n - 2)
    four[3].arrive()
    for k in four:
        k.leave()
    for k in (near, far, near_swap, far_swap):
        k.leave()
    out.wait()


A1, B1, B2 = 3, 6, 9


def layer(x, gain, wq, wk, wv, wo, cos, sin, side):
    total, d = x.shape
    cols = wq.shape[1]
    r, n = CHUNK, total // CHUNK
    quarter = d // 2 // side
    half = quarter // 2
    rows = r // side
    vmem = lambda *s: pltpu.VMEM(s, jnp.bfloat16)
    wide = lambda *s: pltpu.VMEM(s, jnp.float32)
    dma = lambda *s: pltpu.SemaphoreType.DMA(s)
    whole = pl.BlockSpec(memory_space=pltpu.VMEM)
    return pl.pallas_call(
        functools.partial(_layer, side=side),
        in_specs=[ANY, whole, ANY, ANY, ANY, ANY, whole, whole],
        out_specs=[ANY] * 4,
        out_shape=[
            _bf16(n - 1, side, side, rows, quarter), _bf16(n - 1, side, side, rows, quarter), _bf16(2, rows, quarter),
            _bf16(2, 2, side - 1, cols, half),
        ],
        scratch_shapes=[
            vmem(2, PIECE, d), vmem(r, d), vmem(SLOTS, DEEP, 3 * cols), wide(r, 3 * cols),
            vmem(r, cols), vmem(total, cols), vmem(total, cols), wide(cols // HEAD, r), wide(cols // HEAD, HEAD + 8, r),
            vmem(2, 2, side, r, cols), wide(2, rows, quarter), vmem(2, side - 1, rows, quarter), vmem(2, 2, side - 1, rows, quarter),
            vmem(2, rows, quarter), vmem(2, rows, quarter),
            dma(2), dma(SLOTS, 3), dma(2), dma(2), dma(2, 3), dma(2, 3), dma(2, 3), dma(2, 3),
            dma(2, 2, 4), dma(2, 2, 4), dma(2, 2, 3), dma(2, 2, 3), dma(2, 2, 8), dma(2, 2, 8),
        ],
        compiler_params=_params(collective_id=0, has_side_effects=True),
        cost_estimate=pl.CostEstimate(flops=8 * total * d * cols, transcendentals=0, bytes_accessed=8 * d * cols * n),
        name="layer",
    )(x, gain, wq, wk, wv, wo, cos, sin)


def _lay_all(g0_ref, g1_ref, y_ref, buf, in_sem, out_sem, *, side):
    n, _, _, rows, quarter = g0_ref.shape

    def ins(c):
        slot = lax.rem(c, 2)
        return [pltpu.make_async_copy(g.at[c], buf.at[slot, a], in_sem.at[slot, a]) for a, g in enumerate((g0_ref, g1_ref))]

    def outs(c):
        slot = lax.rem(c, 2)
        return [
            pltpu.make_async_copy(
                buf.at[slot, a, i, j],
                y_ref.at[pl.ds(pl.multiple_of((c * side + i) * rows, rows), rows), pl.ds((a * side + j) * quarter, quarter)],
                out_sem.at[slot, a, i, j],
            )
            for a in range(2) for i in range(side) for j in range(side)
        ]

    for c in ins(0):
        c.start()

    def one(c, _):
        @pl.when(c > 0)
        def _():
            for k in outs(c - 1):
                k.wait()

        @pl.when(c + 1 < n)
        def _():
            for k in ins(c + 1):
                k.start()

        for k in ins(c):
            k.wait()
        for k in outs(c):
            k.start()

    lax.fori_loop(0, n, one, None)
    for k in outs(n - 1):
        k.wait()


def lay_all(g0, g1, shape, side):
    return pl.pallas_call(
        functools.partial(_lay_all, side=side),
        in_specs=[ANY, ANY],
        out_specs=ANY,
        out_shape=_bf16(*shape),
        scratch_shapes=[
            pltpu.VMEM((2, 2, *g0.shape[1:]), jnp.bfloat16), pltpu.SemaphoreType.DMA((2, 2)), pltpu.SemaphoreType.DMA((2, 2, side, side)),
        ],
        compiler_params=_params(),
        cost_estimate=pl.CostEstimate(flops=400 * g0.size, transcendentals=0, bytes_accessed=8 * g0.size),
        name="lay_all",
    )(g0, g1)


def _lay(got_ref, *rest, side, start):
    y_ref, buf, in_sem, out_sem = rest[-4:]
    n, _, rows, quarter = got_ref.shape

    def spot(t, a):
        i, j = t // side, t % side
        i, j = (j, i) if a == 0 else (i, side + j)
        return y_ref.at[pl.ds(start + i * rows, rows), pl.ds(j * quarter, quarter)]

    ins = [pltpu.make_async_copy(got_ref.at[t], buf.at[t], in_sem.at[t]) for t in range(n)]
    outs = [pltpu.make_async_copy(buf.at[t, a], spot(t, a), out_sem.at[t, a]) for t in range(n) for a in range(2)]
    for c in ins:
        c.start()
    for t in range(n):
        ins[t].wait()
        outs[2 * t].start()
        outs[2 * t + 1].start()
    for c in outs:
        c.wait()


def lay(got, y, shape, start, side):
    first = y is None
    n = got.shape[0]
    return pl.pallas_call(
        functools.partial(_lay, side=side, start=start),
        in_specs=[ANY] * (1 if first else 2),
        out_specs=ANY,
        out_shape=_bf16(*shape),
        scratch_shapes=[pltpu.VMEM(got.shape, jnp.bfloat16), pltpu.SemaphoreType.DMA((n,)), pltpu.SemaphoreType.DMA((n, 2))],
        input_output_aliases={} if first else {1: 0},
        compiler_params=_params(),
        cost_estimate=pl.CostEstimate(flops=400 * got.size, transcendentals=0, bytes_accessed=4 * got.size),
        name=f"lay_{start}",
    )(got, *(() if first else (y,)))


def solution(mesh):
    side = math.isqrt(mesh.shape["tp"])

    def step(x, gain, wq, wk, wv, wo):
        rows = x.shape[0]
        angle = jnp.arange(rows, dtype=jnp.float32)[:, None] * THETA ** (-jnp.arange(HEAD // 2, dtype=jnp.float32) / (HEAD // 2))
        cos, sin = jnp.cos(angle), jnp.sin(angle)
        cos, sin = jnp.concatenate([cos, cos], 1), jnp.concatenate([-sin, sin], 1)
        g0, g1, last, _ = layer(x, gain[None], wq, wk, wv, wo, cos, sin, side)
        got = lax.all_gather(last, "tp")
        return lay(got, lay_all(g0, g1, x.shape, side), x.shape, rows - CHUNK, side)

    tokens, columns = P("dp", None), P(None, "tp")
    return jax.shard_map(
        step,
        mesh=mesh,
        in_specs=(tokens, P(None), columns, columns, columns, P("tp", None)),
        out_specs=tokens,
        check_vma=False,
    )
```

```python
import functools
import math

import jax
import jax.numpy as jnp
from jax import lax
from jax.experimental import pallas as pl
from jax.experimental.pallas import tpu as pltpu
from jax.sharding import PartitionSpec as P

HEAD = 128
THETA = 10000
NEG = -1e30
HIDDEN = 2 * NEG
LOG2E = 1.4426950408889634
VMEM = 63 * 2**20
CHUNK = 256
PIECE = 32
DEEP = 1792
ANY = pl.BlockSpec(memory_space=pl.ANY)
MESH = pl.DeviceIdType.MESH


def _dot(a, b, ca=1, cb=0):
    return lax.dot_general(a, b, (((ca,), (cb,)), ((), ())), preferred_element_type=jnp.float32)


def _params(**kw):
    return pltpu.CompilerParams(vmem_limit_bytes=VMEM, **kw)


def _bf16(*shape):
    return jax.ShapeDtypeStruct(shape, jnp.bfloat16)


def _times(n, size):
    return pl.ds(pl.multiple_of(n * size, size), size)


class Copies:
    def __init__(self, make):
        self.make = make

    def start(self):
        for c in self.make():
            c.start()

    def arrive(self):
        for c in self.make():
            c.wait_recv()

    def leave(self):
        for c in self.make():
            c.wait_send()


def _layer(x_ref, gain_ref, wq_ref, wk_ref, wv_ref, wo_ref, ca_ref, sa_ref, cb_ref, sb_ref, g0_ref, g1_ref, cut_ref, way_ref,
           xin, a_s, w_s, acc, q_s, k_s, v_s, top_s, mix_s, s_s, keep_s, send_s, recv_s, res_s, blk_s,
           x_sem, w_sem, res_sem, blk_sem, hop_send, hop_recv, cut_send, cut_recv, swap_send, swap_recv,
           ring_send, ring_recv, sum_send, sum_recv, all_send, all_recv, *, side):
    total_rows, d = x_ref.shape
    cols = wq_ref.shape[1]
    r, n = CHUNK, total_rows // CHUNK
    heads = cols // HEAD
    width = d // 2 // side
    half = width // 2
    rows = r // side
    steps = d // DEEP
    t, dp = lax.axis_index("tp"), lax.axis_index("dp")
    x, y = lax.div(t, side), lax.rem(t, side)
    core = lax.rem(dp, 2)
    g_ref = (g0_ref, g1_ref)

    def at(i, j):
        return {"tp": lax.rem(i, side) * side + lax.rem(j, side)}

    def along(a, k):
        return at(x + (1 - a) * k, y + a * k)

    place = (x, y)
    ends = [(along(a, 1), along(a, side - 1)) for a in range(2)]
    col0 = lambda a, at: pl.multiple_of((a * side + at) * width, 128)
    sibling = {"dp": dp + 1 - 2 * core}

    def remote(src, dst, send, recv, to):
        return pltpu.make_async_remote_copy(src, dst, send, recv, device_id=to, device_id_type=MESH)

    h = cols // 2
    rows_of = lambda b: pl.ds(b * h, h)

    def wo_cols(a, k):
        return pl.ds(pl.multiple_of(col0(a, lax.rem(place[a] + k, side)) + core * half, 128), half)

    def hop():
        return Copies(lambda: [
            remote(wo_ref.at[rows_of(b), wo_cols(a, 2)], way_ref.at[a, b], hop_send.at[a, b], hop_recv.at[a, b], ends[a][b])
            for a in range(2) for b in range(2)
        ])

    def on():
        return Copies(lambda: [
            remote(way_ref.at[a, b], cut_ref.at[a, 0, 2, rows_of(b)], cut_send.at[a, 2 + b], cut_recv.at[a, 2 + b], ends[a][b])
            for a in range(2) for b in range(2)
        ])

    def near():
        return Copies(lambda: [
            remote(wo_ref.at[:, wo_cols(a, k)], cut_ref.at[a, 0, b], cut_send.at[a, b], cut_recv.at[a, b], ends[a][b])
            for a in range(2) for b, k in enumerate((1, side - 1))
        ])

    def swap(places):
        return Copies(lambda: [
            remote(cut_ref.at[a, 0, i], cut_ref.at[a, 1, i], swap_send.at[a, i], swap_recv.at[a, i], sibling) for a in range(2) for i in places
        ])

    near_swap, far_swap = swap((0, 1)), swap((2,))

    def ring(c):
        slot = lax.rem(c, 2)
        h = r // 2

        def make(later):
            out = []
            for a in range(2):
                here = lambda j, first=0, size=r: s_s.at[slot, a, pl.ds(first, size), pl.ds(j * cols, cols)]
                for b in range(2):
                    src, dst = (here(1 + b, b * h, h), here(3, b * h, h)) if later else (here(0), here(1 + b))
                    i = 2 * later + b
                    out.append(remote(src, dst, ring_send.at[slot, a, i], ring_recv.at[slot, a, i], ends[a][b]))
            return out

        return Copies(lambda: make(0)), Copies(lambda: make(1))

    def everywhere(c, a):
        slot = lax.rem(c, 4)
        h, m = rows // 2, side // 2
        g = g_ref[a].at[c]
        i, j = place[1 - a], place[a]
        pair = lambda ref, k, to: remote(ref, ref, all_send.at[slot, a, k], all_recv.at[slot, a, k], to)
        up, down = ends[a]
        back, ahead = lax.rem(j + side - 1, side), lax.rem(j + 1, side)
        one = Copies(lambda: [pair(g.at[i, j], 0, up), pair(g.at[i, j], 1, down)])
        two = Copies(lambda: [pair(g.at[i, back, pl.ds(0, h)], 2, up), pair(g.at[i, ahead, pl.ds(h, h)], 3, down)])
        up_, down_ = ends[1 - a]
        back_, ahead_ = lax.rem(i + side - 1, side), lax.rem(i + 1, side)
        three = Copies(lambda: [pair(g.at[i], 4, up_), pair(g.at[i], 5, down_)])
        four = Copies(lambda: [pair(g.at[back_, pl.ds(0, m)], 6, up_), pair(g.at[ahead_, pl.ds(m, m)], 7, down_)])
        return one, two, three, four

    def x_copy(c, i):
        slot = lax.rem(i, 2)
        return pltpu.make_async_copy(x_ref.at[pl.ds(pl.multiple_of(c * r + i * PIECE, PIECE), PIECE)], xin.at[slot], x_sem.at[slot])

    def w_copies(i):
        slot = lax.rem(i, 2)
        return [
            pltpu.make_async_copy(w.at[_times(i, DEEP)], w_s.at[slot, :, pl.ds(k * cols, cols)], w_sem.at[slot, k])
            for k, w in enumerate((wq_ref, wk_ref, wv_ref))
        ]

    def o_copies(a, kh):
        out = []
        for j in (2 * kh, 2 * kh + 1):
            here = w_s.at[kh, pl.ds((j % 2) * cols, cols)]
            if j == 0:
                mine = wo_ref.at[:, pl.ds(col0(a, place[a]), width)]
                out.append(pltpu.make_async_copy(mine, here.at[:, pl.ds(0, width)], w_sem.at[kh, 0]))
                continue
            for b in range(2):
                first = pl.multiple_of(lax.rem(core + b, 2) * half, 128)
                out.append(pltpu.make_async_copy(cut_ref.at[a, b, j - 1], here.at[:, pl.ds(first, half)], w_sem.at[kh, (j % 2) * 2 + b]))
        return out

    def go(copies):
        for c in copies:
            c.start()

    def done(copies):
        for c in copies:
            c.wait()

    def sums(c, a):
        slot = lax.rem(c, 2)
        sem = lambda m: (sum_send.at[slot, a, m], sum_recv.at[slot, a, m])
        first = Copies(lambda: [
            remote(send_s.at[a, b], recv_s.at[slot, a, b], *sem(b), to) for b, to in enumerate(ends[1 - a])
        ])
        second = Copies(lambda: [
            remote(send_s.at[a, 2, :, pl.ds(b * half, half)], recv_s.at[slot, a, 2, :, pl.ds(b * half, half)], *sem(2 + b), to)
            for b, to in enumerate(ends[1 - a])
        ])
        return first, second

    def residual(c, a):
        return [pltpu.make_async_copy(
            x_ref.at[pl.ds(pl.multiple_of(c * r + place[1 - a] * rows, rows), rows), pl.ds(col0(a, place[a]), width)],
            res_s.at[a], res_sem.at[a])]

    def block_copies(c, a):
        return [pltpu.make_async_copy(blk_s.at[a], g_ref[a].at[c, place[1 - a], place[a]], blk_sem.at[a])]

    def norm(p):
        def piece(i, _):
            x_copy(p, i).wait()
            slot = lax.rem(i, 2)
            total = jnp.zeros((PIECE, HEAD), jnp.float32)
            for k in range(0, d, HEAD):
                wide = xin[slot, :, k : k + HEAD].astype(jnp.float32)
                total += wide * wide
            scale = lax.rsqrt(jnp.sum(total, -1, keepdims=True) * (1 / d) + 1e-6)
            here = _times(i, PIECE)
            for k in range(0, d, 4 * HEAD):
                at = slice(k, k + 4 * HEAD)
                wide = xin[slot, :, at].astype(jnp.float32)
                a_s[here, at] = (wide * scale * gain_ref[:, at].astype(jnp.float32)).astype(jnp.bfloat16)

            @pl.when(i + 2 < r // PIECE)
            def _():
                x_copy(p, i + 2).start()

        lax.fori_loop(0, r // PIECE, piece, None)

    def project(p, hooks):
        def at_step(i, _):
            pl.when(i + 1 < steps)(lambda: go(w_copies(i + 1)))
            hooks(i)
            pl.when((i + 1 == steps) & (p > 0))(lambda: go(o_copies(0, 0)))
            done(w_copies(i))
            got = _dot(a_s[:, _times(i, DEEP)], w_s[lax.rem(i, 2)])

            @pl.when(i == 0)
            def _():
                acc[...] = got

            @pl.when(i > 0)
            def _():
                acc[...] += got

        lax.fori_loop(0, steps, at_step, None)
        here = _times(p, r)
        ca, sa, cb, sb = ca_ref[pl.ds(p, 1), :], sa_ref[pl.ds(p, 1), :], cb_ref[...], sb_ref[...]
        cos, sin = ca * cb - sa * sb, sa * cb + ca * sb
        turn = lambda t: (t * cos + pltpu.roll(t, HEAD // 2, 1) * sin).astype(jnp.bfloat16)
        for h in range(heads):
            a = slice(h * HEAD, (h + 1) * HEAD)
            q_s[:, a] = turn(acc[:, a].astype(jnp.bfloat16).astype(jnp.float32))
            k_s[here, a] = turn(acc[:, cols + h * HEAD : cols + (h + 1) * HEAD].astype(jnp.bfloat16).astype(jnp.float32))
        v_s[here, :] = acc[:, 2 * cols :].astype(jnp.bfloat16)

    def attend(p):
        e = HEAD**-0.5 * LOG2E
        top_s[...] = jnp.full(top_s.shape, NEG, jnp.float32)
        mix_s[...] = jnp.zeros(mix_s.shape, jnp.float32)
        ones = jnp.ones((8, r), jnp.bfloat16)

        def block(j, masked):
            here = _times(j, r)
            scores = [_dot(k_s[here, h * HEAD : (h + 1) * HEAD], q_s[:, h * HEAD : (h + 1) * HEAD], 1, 1) for h in range(heads)]
            if masked:
                ok = lax.broadcasted_iota(jnp.int32, (r, r), 1) >= lax.broadcasted_iota(jnp.int32, (r, r), 0)
            weights, keeps = [], []
            for h, s in enumerate(scores):
                if masked:
                    s = jnp.where(ok, s, HIDDEN)
                old = top_s[h : h + 1, :]
                top = jnp.maximum(old, s.max(axis=0, keepdims=True))
                top_s[h : h + 1, :] = top
                weights.append(jnp.exp2((s - top) * e).astype(jnp.bfloat16))
                keeps.append(jnp.exp2((old - top) * e))
            for h, (w, keep) in enumerate(zip(weights, keeps)):
                values = jnp.concatenate([v_s[here, h * HEAD : (h + 1) * HEAD].T, ones], axis=0)
                mix_s[h] = mix_s[h] * keep + _dot(values, w)

        lax.fori_loop(0, p, lambda j, _: block(j, False), None)
        block(p, True)
        slot = lax.rem(p, 2)
        for h in range(heads):
            got = (mix_s[h, :HEAD, :] * (1 / mix_s[h, HEAD : HEAD + 1, :])).T.astype(jnp.bfloat16)
            for a in range(2):
                s_s[slot, a, :, h * HEAD : (h + 1) * HEAD] = got

    def product(c, a, before, after):
        slot = lax.rem(c, 2)
        for kh, then in enumerate((before, after)):
            then()
            done(o_copies(a, kh))
            got = _dot(s_s[slot, a, :, kh * DEEP : (kh + 1) * DEEP], w_s[kh, :, :width])
            if kh == 0:
                acc[:, :width] = got
            else:
                acc[:, :width] += got
        one, two = slice(0, half), slice(half, width)
        piece = lambda k, at: acc[_times(lax.rem(place[1 - a] + k, side), rows), at]
        for b, (k, l) in enumerate(((2, 1), (3, 2))):
            send_s[a, b, :, one] = piece(k, one).astype(jnp.bfloat16)
            send_s[a, b, :, two] = piece(l, two).astype(jnp.bfloat16)
        sums(c, a)[0].start()
        keep_s[a, 0] = piece(0, slice(0, width))
        keep_s[a, 1, :, one] = piece(1, one)
        keep_s[a, 1, :, two] = piece(3, two)

    def sum_on(c, a):
        slot = lax.rem(c, 2)
        first, second = sums(c, a)
        first.arrive()
        for b in range(2):
            at = slice(b * half, (b + 1) * half)
            send_s[a, 2, :, at] = (keep_s[a, 1, :, at] + recv_s[slot, a, b, :, at].astype(jnp.float32)).astype(jnp.bfloat16)
        second.start()

    def finish(c, a):
        slot = lax.rem(c, 2)
        first, second = sums(c, a)
        done(residual(c, a))
        second.arrive()
        for b in range(2):
            at = slice(b * half, (b + 1) * half)
            wide = lambda ref: ref.astype(jnp.float32)
            total = keep_s[a, 0, :, at] + wide(recv_s[slot, a, 1 - b, :, at]) + wide(recv_s[slot, a, 2, :, at])
            blk_s[a, :, at] = (wide(res_s[a, :, at]) + total).astype(jnp.bfloat16)
        first.leave()
        second.leave()

    for i in range(2):
        x_copy(0, i).start()
    go(w_copies(0))
    peers = [along(a, k) for a in range(2) for k in range(1, side)] + [sibling]
    barrier = pltpu.get_barrier_semaphore()
    for k in peers:
        pl.semaphore_signal(barrier, inc=1, device_id=k, device_id_type=MESH)
    pl.semaphore_wait(barrier, len(peers))
    hop().start()
    near().start()

    def sum_end(c, a):
        finish(c, a)
        go(block_copies(c, a))

    def gather_one(c, a):
        done(block_copies(c, a))
        everywhere(c, a)[0].start()

    def gather_two(c, a):
        one, two, _, _ = everywhere(c, a)
        one.arrive()
        two.start()

    def gather_three(c, a):
        _, two, three, _ = everywhere(c, a)
        two.arrive()
        three.start()

    def gather_four(c, a):
        _, _, three, four = everywhere(c, a)
        three.arrive()
        four.start()

    def gather_end(c, a):
        all_ = everywhere(c, a)
        all_[3].arrive()
        for k in all_:
            k.leave()

    stages = dict(on=sum_on, end=sum_end, one=gather_one, two=gather_two, three=gather_three, four=gather_four, last=gather_end)

    def relay(p):
        first, second = ring(p - 1)
        first.arrive()
        second.start()

    def project_out(c, late, then, between=lambda: None):
        def before_0():
            late()
            go(o_copies(0, 1))

        product(c, 0, before_0, lambda: go(o_copies(1, 0)))
        between()
        product(c, 1, lambda: go(o_copies(1, 1)), then)
        for k in ring(c):
            k.leave()

    def period(p, _):
        def stage(name, a, lag):
            c = p - lag - 1
            pl.when(c >= 0)(lambda: stages[name](c, a))

        def hooks(i):
            for a in range(2):
                for name, at in zip(STAGES, HOOKS[a]):
                    lag, when = divmod(at, PLACES)
                    if isinstance(i, int):
                        if i == when:
                            stage(name, a, lag)
                    elif 1 <= when <= steps:
                        pl.when(i == when)(functools.partial(stage, name, a, lag))

        def early(i, k, when, *todo):
            @pl.when((p == k) & (i == when))
            def _():
                for f in todo:
                    f()

        def inner(i):
            early(i, 0, 5, hop().arrive, on().start)
            early(i, 1, 5, near().arrive, near_swap.start)
            early(i, 1, steps, near_swap.arrive)
            for k, when in enumerate(RELAYS, 2):
                here = (p == k) if k < len(RELAYS) + 1 else (p >= k)
                pl.when(here & (i == when))(lambda: relay(p))
            hooks(i)

        @pl.when(p > 0)
        def _():
            ring(p - 1)[0].start()

        @pl.when(p > 1)
        def _():
            for a in range(2):
                go(residual(p - 2, a))

        hooks(0)
        norm(p)

        @pl.when(p + 1 < n)
        def _():
            for i in range(2):
                x_copy(p + 1, i).start()

        project(p, lambda i: inner(i + 1))

        @pl.when(p == 1)
        def _():
            on().arrive()
            far_swap.start()
            relay(p)

        hooks(steps + 1)

        def next_period():
            pl.when(p + 1 < n)(lambda: go(w_copies(0)))

        pl.when(p == 0)(next_period)

        @pl.when(p > 0)
        def _():
            ring(p - 1)[1].arrive()
            project_out(p - 1, lambda: pl.when(p == 1)(far_swap.arrive), next_period, lambda: hooks(steps + 2))

        hooks(steps + 3)
        attend(p)
        hooks(steps + 4)

    lax.fori_loop(0, n, period, None)
    go(o_copies(0, 0))
    ring(n - 1)[0].start()
    for a in range(2):
        go(residual(n - 2, a))
    for name, back, a in TAIL:
        if name == "relay":
            relay(n)
        elif name == "product":
            ring(n - 1)[1].arrive()
            project_out(n - 1, lambda: None, lambda: None)
            for b in range(2):
                go(residual(n - 1, b))
        else:
            stages[name](n - back, a)
    for k in (hop(), on(), near(), near_swap, far_swap):
        k.leave()


STAGES = ("on", "end", "one", "two", "three", "four", "last")
PLACES = 13
HOOKS = ((14, 18, 19, 23, 28, 34, 48), (14, 17, 21, 24, 28, 35, 43))
RELAYS = (5, 3, 4)
TAIL = (
    ("on", 2, 0), ("three", 3, 0), ("three", 3, 1), ("last", 4, 0), ("last", 4, 1), ("on", 2, 1), ("relay", 0, 0), ("end", 2, 0),
    ("one", 2, 0), ("four", 3, 1), ("four", 3, 0), ("end", 2, 1), ("one", 2, 1), ("product", 0, 0), ("two", 2, 0), ("last", 3, 0),
    ("two", 2, 1), ("last", 3, 1), ("on", 1, 0), ("on", 1, 1), ("three", 2, 1), ("three", 2, 0), ("end", 1, 0), ("end", 1, 1),
    ("one", 1, 0), ("one", 1, 1), ("four", 2, 0), ("four", 2, 1), ("two", 1, 1), ("two", 1, 0), ("last", 2, 0), ("last", 2, 1),
    ("three", 1, 1), ("three", 1, 0), ("four", 1, 1), ("four", 1, 0), ("last", 1, 1), ("last", 1, 0),
)


def layer(x, gain, wq, wk, wv, wo, tables, side):
    total, d = x.shape
    cols = wq.shape[1]
    r, n = CHUNK, total // CHUNK
    width = d // 2 // side
    rows = r // side
    vmem = lambda *s: pltpu.VMEM(s, jnp.bfloat16)
    wide = lambda *s: pltpu.VMEM(s, jnp.float32)
    dma = lambda *s: pltpu.SemaphoreType.DMA(s)
    whole = pl.BlockSpec(memory_space=pltpu.VMEM)
    blocks = _bf16(n, side, side, rows, width)
    return pl.pallas_call(
        functools.partial(_layer, side=side),
        in_specs=[ANY, whole, ANY, ANY, ANY, ANY] + [whole] * 4,
        out_specs=[ANY] * 4,
        out_shape=[blocks, blocks, _bf16(2, 2, side - 1, cols, width // 2), _bf16(2, 2, cols // 2, width // 2)],
        scratch_shapes=[
            vmem(2, PIECE, d), vmem(r, d), vmem(2, DEEP, 3 * cols), wide(r, 3 * cols),
            vmem(r, cols), vmem(total, cols), vmem(total, cols), wide(cols // HEAD, r), wide(cols // HEAD, HEAD + 8, r),
            vmem(2, 2, r, side * cols), wide(2, 2, rows, width), vmem(2, 3, rows, width), vmem(2, 2, 3, rows, width),
            vmem(2, rows, width), vmem(2, rows, width),
            dma(2), dma(2, 4), dma(2), dma(2), dma(2, 2), dma(2, 2), dma(2, 4), dma(2, 4), dma(2, 3), dma(2, 3),
            dma(2, 2, 4), dma(2, 2, 4), dma(2, 2, 4), dma(2, 2, 4), dma(4, 2, 8), dma(4, 2, 8),
        ],
        compiler_params=_params(collective_id=0, has_side_effects=True),
        cost_estimate=pl.CostEstimate(flops=8 * total * d * cols, transcendentals=0, bytes_accessed=8 * d * cols * n),
        name="layer",
    )(x, gain, wq, wk, wv, wo, *tables)


def _lay(g0_ref, g1_ref, y_ref, buf, in_sem, out_sem, *, side):
    n, _, _, rows, width = g0_ref.shape

    def ins(c):
        slot = lax.rem(c, 2)
        return [pltpu.make_async_copy(g.at[c], buf.at[slot, a], in_sem.at[slot, a]) for a, g in enumerate((g0_ref, g1_ref))]

    def outs(c):
        slot = lax.rem(c, 2)
        return [
            pltpu.make_async_copy(
                buf.at[slot, a, i, j],
                y_ref.at[pl.ds(pl.multiple_of((c * side + i) * rows, rows), rows), pl.ds((a * side + j) * width, width)],
                out_sem.at[slot, a, i, j],
            )
            for a in range(2) for i in range(side) for j in range(side)
        ]

    for c in ins(0):
        c.start()

    def one(c, _):
        @pl.when(c > 0)
        def _():
            for k in outs(c - 1):
                k.wait()

        @pl.when(c + 1 < n)
        def _():
            for k in ins(c + 1):
                k.start()

        for k in ins(c):
            k.wait()
        for k in outs(c):
            k.start()

    lax.fori_loop(0, n, one, None)
    for k in outs(n - 1):
        k.wait()


def lay(g0, g1, shape, side):
    return pl.pallas_call(
        functools.partial(_lay, side=side),
        in_specs=[ANY, ANY],
        out_specs=ANY,
        out_shape=_bf16(*shape),
        scratch_shapes=[
            pltpu.VMEM((2, 2, *g0.shape[1:]), jnp.bfloat16),
            pltpu.SemaphoreType.DMA((2, 2)), pltpu.SemaphoreType.DMA((2, 2, side, side)),
        ],
        compiler_params=_params(),
        cost_estimate=pl.CostEstimate(flops=400 * g0.size, transcendentals=0, bytes_accessed=4 * (g0.size + g1.size)),
        name="lay",
    )(g0, g1)


def solution(mesh):
    side = math.isqrt(mesh.shape["tp"])

    def step(x, gain, wq, wk, wv, wo):
        rows = x.shape[0]

        def table(places):
            angle = places.astype(jnp.float32)[:, None] * THETA ** (-(jnp.arange(HEAD) % (HEAD // 2)).astype(jnp.float32) / (HEAD // 2))
            return jnp.cos(angle), jnp.where(jnp.arange(HEAD) < HEAD // 2, -jnp.sin(angle), jnp.sin(angle))

        tables = *table(jnp.arange(0, rows, CHUNK)), *table(jnp.arange(CHUNK))
        g0, g1, *_ = layer(x, gain[None], wq, wk, wv, wo, tables, side)
        return lay(g0, g1, x.shape, side)

    tokens, columns = P("dp", None), P(None, "tp")
    return jax.shard_map(
        step,
        mesh=mesh,
        in_specs=(tokens, P(None), columns, columns, columns, P("tp", None)),
        out_specs=tokens,
        check_vma=False,
    )
```

```python
import functools
import math

import jax
import jax.numpy as jnp
import numpy as np
from jax import lax
from jax.experimental import pallas as pl
from jax.experimental.pallas import tpu as pltpu
from jax.sharding import PartitionSpec as P

HEAD = 128
THETA = 10000
NEG = -1e30
HIDDEN = 2 * NEG
LOG2E = 1.4426950408889634
VMEM = 67_000_000
CHUNK = 256
PIECE = 32
DEEP = 1792
ANY = pl.BlockSpec(memory_space=pl.ANY)
MESH = pl.DeviceIdType.MESH


def _dot(a, b, ca=1, cb=0):
    return lax.dot_general(a, b, (((ca,), (cb,)), ((), ())), preferred_element_type=jnp.float32)


def _params(**kw):
    return pltpu.CompilerParams(vmem_limit_bytes=VMEM, **kw)


def _bf16(*shape):
    return jax.ShapeDtypeStruct(shape, jnp.bfloat16)


def _times(n, size):
    return pl.ds(pl.multiple_of(n * size, size), size)


class Copies:
    def __init__(self, make):
        self.make = make

    def start(self):
        for c in self.make():
            c.start()

    def arrive(self):
        for c in self.make():
            c.wait_recv()

    def leave(self):
        for c in self.make():
            c.wait_send()


def _layer(x_ref, gain_ref, wq_ref, wk_ref, wv_ref, wo_ref, ca_ref, sa_ref, cb_ref, sb_ref, g0_ref, g1_ref, cut_ref, way_ref,
           xin, a_s, w_s, acc, q_s, k_s, v_s, top_s, mix_s, s_s, keep_s, send_s, recv_s, res_s, blk_s,
           x_sem, w_sem, res_sem, blk_sem, hop_send, hop_recv, cut_send, cut_recv, swap_send, swap_recv,
           ring_send, ring_recv, sum_send, sum_recv, all_send, all_recv, *, side):
    total_rows, d = x_ref.shape
    cols = wq_ref.shape[1]
    r, n = CHUNK, total_rows // CHUNK
    heads = cols // HEAD
    width = d // 2 // side
    half = width // 2
    rows = r // side
    steps = d // DEEP
    t, dp = lax.axis_index("tp"), lax.axis_index("dp")
    x, y = lax.div(t, side), lax.rem(t, side)
    core = lax.rem(dp, 2)
    g_ref = (g0_ref, g1_ref)

    def at(i, j):
        return {"tp": lax.rem(i, side) * side + lax.rem(j, side)}

    def along(a, k):
        return at(x + (1 - a) * k, y + a * k)

    place = (x, y)
    ends = [(along(a, 1), along(a, side - 1)) for a in range(2)]
    col0 = lambda a, at: pl.multiple_of((a * side + at) * width, 128)
    sibling = {"dp": dp + 1 - 2 * core}

    def remote(src, dst, send, recv, to):
        return pltpu.make_async_remote_copy(src, dst, send, recv, device_id=to, device_id_type=MESH)

    h = cols // 2
    rows_of = lambda b: pl.ds(b * h, h)

    def wo_cols(a, k):
        return pl.ds(pl.multiple_of(col0(a, lax.rem(place[a] + k, side)) + core * half, 128), half)

    def hop():
        return Copies(lambda: [
            remote(wo_ref.at[rows_of(b), wo_cols(a, 2)], way_ref.at[a, b], hop_send.at[a, b], hop_recv.at[a, b], ends[a][b])
            for a in range(2) for b in range(2)
        ])

    def on():
        return Copies(lambda: [
            remote(way_ref.at[a, b], cut_ref.at[a, 0, 2, rows_of(b)], cut_send.at[a, 2 + b], cut_recv.at[a, 2 + b], ends[a][b])
            for a in range(2) for b in range(2)
        ])

    def near():
        return Copies(lambda: [
            remote(wo_ref.at[:, wo_cols(a, k)], cut_ref.at[a, 0, b], cut_send.at[a, b], cut_recv.at[a, b], ends[a][b])
            for a in range(2) for b, k in enumerate((1, side - 1))
        ])

    def swap(places):
        return Copies(lambda: [
            remote(cut_ref.at[a, 0, i], cut_ref.at[a, 1, i], swap_send.at[a, i], swap_recv.at[a, i], sibling) for a in range(2) for i in places
        ])

    near_swap, far_swap = swap((0, 1)), swap((2,))

    def ring(c):
        slot = lax.rem(c, 3)
        h = r // 2

        def make(later):
            out = []
            for a in range(2):
                here = lambda j, first=0, size=r: s_s.at[slot, a, pl.ds(first, size), pl.ds(j * cols, cols)]
                for b in range(2):
                    src, dst = (here(1 + b, b * h, h), here(3, b * h, h)) if later else (here(0), here(1 + b))
                    i = 2 * later + b
                    out.append(remote(src, dst, ring_send.at[slot, a, i], ring_recv.at[slot, a, i], ends[a][b]))
            return out

        return Copies(lambda: make(0)), Copies(lambda: make(1))

    def everywhere(c, a):
        slot = lax.rem(c, 4)
        h, m = rows // 2, side // 2
        g = g_ref[a].at[c]
        i, j = place[1 - a], place[a]
        pair = lambda ref, k, to: remote(ref, ref, all_send.at[slot, a, k], all_recv.at[slot, a, k], to)
        up, down = ends[a]
        back, ahead = lax.rem(j + side - 1, side), lax.rem(j + 1, side)
        one = Copies(lambda: [pair(g.at[i, j], 0, up), pair(g.at[i, j], 1, down)])
        two = Copies(lambda: [pair(g.at[i, back, pl.ds(0, h)], 2, up), pair(g.at[i, ahead, pl.ds(h, h)], 3, down)])
        up_, down_ = ends[1 - a]
        back_, ahead_ = lax.rem(i + side - 1, side), lax.rem(i + 1, side)
        three = Copies(lambda: [pair(g.at[i], 4, up_), pair(g.at[i], 5, down_)])
        four = Copies(lambda: [pair(g.at[back_, pl.ds(0, m)], 6, up_), pair(g.at[ahead_, pl.ds(m, m)], 7, down_)])
        return one, two, three, four

    def x_copy(c, i):
        slot = lax.rem(i, 2)
        return pltpu.make_async_copy(x_ref.at[pl.ds(pl.multiple_of(c * r + i * PIECE, PIECE), PIECE)], xin.at[slot], x_sem.at[slot])

    def w_copies(i):
        slot = lax.rem(i, 2)
        return [
            pltpu.make_async_copy(w.at[_times(i, DEEP)], w_s.at[slot, :, pl.ds(k * cols, cols)], w_sem.at[slot, k])
            for k, w in enumerate((wq_ref, wk_ref, wv_ref))
        ]

    def o_copies(a, kh):
        out = []
        for j in (2 * kh, 2 * kh + 1):
            here = w_s.at[kh, pl.ds((j % 2) * cols, cols)]
            if j == 0:
                mine = wo_ref.at[:, pl.ds(col0(a, place[a]), width)]
                out.append(pltpu.make_async_copy(mine, here.at[:, pl.ds(0, width)], w_sem.at[kh, 0]))
                continue
            for b in range(2):
                first = pl.multiple_of(lax.rem(core + b, 2) * half, 128)
                out.append(pltpu.make_async_copy(cut_ref.at[a, b, j - 1], here.at[:, pl.ds(first, half)], w_sem.at[kh, (j % 2) * 2 + b]))
        return out

    def go(copies):
        for c in copies:
            c.start()

    def done(copies):
        for c in copies:
            c.wait()

    def sums(c, a):
        slot = lax.rem(c, 2)
        sem = lambda m: (sum_send.at[slot, a, m], sum_recv.at[slot, a, m])
        first = Copies(lambda: [
            remote(send_s.at[slot, a, b], recv_s.at[slot, a, b], *sem(b), to) for b, to in enumerate(ends[1 - a])
        ])
        second = Copies(lambda: [
            remote(send_s.at[slot, a, 2, :, pl.ds(b * half, half)], recv_s.at[slot, a, 2, :, pl.ds(b * half, half)], *sem(2 + b), to)
            for b, to in enumerate(ends[1 - a])
        ])
        return first, second

    def residual(c, a):
        return [pltpu.make_async_copy(
            x_ref.at[pl.ds(pl.multiple_of(c * r + place[1 - a] * rows, rows), rows), pl.ds(col0(a, place[a]), width)],
            res_s.at[lax.rem(c, 2), a], res_sem.at[lax.rem(c, 2), a])]

    def block_copies(c, a):
        slot = lax.rem(c, 2)
        return [pltpu.make_async_copy(blk_s.at[slot, a], g_ref[a].at[c, place[1 - a], place[a]], blk_sem.at[slot, a])]

    def norm(p):
        def piece(i, _):
            x_copy(p, i).wait()
            slot = lax.rem(i, 2)
            total = jnp.zeros((PIECE, HEAD), jnp.float32)
            for k in range(0, d, HEAD):
                wide = xin[slot, :, k : k + HEAD].astype(jnp.float32)
                total += wide * wide
            scale = lax.rsqrt(jnp.sum(total, -1, keepdims=True) * (1 / d) + 1e-6)
            here = _times(i, PIECE)
            for k in range(0, d, 4 * HEAD):
                at = slice(k, k + 4 * HEAD)
                wide = xin[slot, :, at].astype(jnp.float32)
                a_s[here, at] = (wide * scale * gain_ref[:, at].astype(jnp.float32)).astype(jnp.bfloat16)

            @pl.when(i + 2 < r // PIECE)
            def _():
                x_copy(p, i + 2).start()

        lax.fori_loop(0, r // PIECE, piece, None)

    def project(p, hooks):
        def at_step(i, _):
            pl.when(i + 1 < steps)(lambda: go(w_copies(i + 1)))
            hooks(i)
            pl.when((i + 1 == steps) & (p > 0))(lambda: go(o_copies(0, 0)))
            done(w_copies(i))
            got = _dot(a_s[:, _times(i, DEEP)], w_s[lax.rem(i, 2)])

            @pl.when(i == 0)
            def _():
                acc[...] = got

            @pl.when(i > 0)
            def _():
                acc[...] += got

        lax.fori_loop(0, steps, at_step, None)
        here = _times(p, r)
        ca, sa, cb, sb = ca_ref[pl.ds(p, 1), :], sa_ref[pl.ds(p, 1), :], cb_ref[...], sb_ref[...]
        cos, sin = ca * cb - sa * sb, sa * cb + ca * sb
        turn = lambda t: (t * cos + pltpu.roll(t, HEAD // 2, 1) * sin).astype(jnp.bfloat16)
        for h in range(heads):
            a = slice(h * HEAD, (h + 1) * HEAD)
            q_s[:, a] = turn(acc[:, a].astype(jnp.bfloat16).astype(jnp.float32))
            k_s[here, a] = turn(acc[:, cols + h * HEAD : cols + (h + 1) * HEAD].astype(jnp.bfloat16).astype(jnp.float32))
        v_s[here, :] = acc[:, 2 * cols :].astype(jnp.bfloat16)

    def attend(p):
        e = HEAD**-0.5 * LOG2E
        top_s[...] = jnp.full(top_s.shape, NEG, jnp.float32)
        mix_s[...] = jnp.zeros(mix_s.shape, jnp.float32)
        ones = jnp.ones((8, r), jnp.bfloat16)

        def block(j, masked):
            here = _times(j, r)
            scores = [_dot(k_s[here, h * HEAD : (h + 1) * HEAD], q_s[:, h * HEAD : (h + 1) * HEAD], 1, 1) for h in range(heads)]
            if masked:
                ok = lax.broadcasted_iota(jnp.int32, (r, r), 1) >= lax.broadcasted_iota(jnp.int32, (r, r), 0)
            weights, keeps = [], []
            for h, s in enumerate(scores):
                if masked:
                    s = jnp.where(ok, s, HIDDEN)
                old = top_s[h : h + 1, :]
                top = jnp.maximum(old, s.max(axis=0, keepdims=True))
                top_s[h : h + 1, :] = top
                weights.append(jnp.exp2((s - top) * e).astype(jnp.bfloat16))
                keeps.append(jnp.exp2((old - top) * e))
            for h, (w, keep) in enumerate(zip(weights, keeps)):
                values = jnp.concatenate([v_s[here, h * HEAD : (h + 1) * HEAD].T, ones], axis=0)
                mix_s[h] = mix_s[h] * keep + _dot(values, w)

        lax.fori_loop(0, p, lambda j, _: block(j, False), None)
        block(p, True)
        slot = lax.rem(p, 3)
        for h in range(heads):
            got = (mix_s[h, :HEAD, :] * (1 / mix_s[h, HEAD : HEAD + 1, :])).T.astype(jnp.bfloat16)
            for a in range(2):
                s_s[slot, a, :, h * HEAD : (h + 1) * HEAD] = got

    def product(c, a, before, after):
        slot = lax.rem(c, 3)
        for kh, then in enumerate((before, after)):
            then()
            done(o_copies(a, kh))
            got = _dot(s_s[slot, a, :, kh * DEEP : (kh + 1) * DEEP], w_s[kh, :, :width])
            if kh == 0:
                acc[:, :width] = got
            else:
                acc[:, :width] += got
        slot = lax.rem(c, 2)
        one, two = slice(0, half), slice(half, width)
        piece = lambda k, at: acc[_times(lax.rem(place[1 - a] + k, side), rows), at]
        for b, (k, l) in enumerate(((2, 1), (3, 2))):
            send_s[slot, a, b, :, one] = piece(k, one).astype(jnp.bfloat16)
            send_s[slot, a, b, :, two] = piece(l, two).astype(jnp.bfloat16)
        sums(c, a)[0].start()
        keep_s[slot, a, 0] = piece(0, slice(0, width))
        keep_s[slot, a, 1, :, one] = piece(1, one)
        keep_s[slot, a, 1, :, two] = piece(3, two)

    def sum_on(c, a):
        slot = lax.rem(c, 2)
        first, second = sums(c, a)
        first.arrive()
        for b in range(2):
            at = slice(b * half, (b + 1) * half)
            send_s[slot, a, 2, :, at] = (keep_s[slot, a, 1, :, at] + recv_s[slot, a, b, :, at].astype(jnp.float32)).astype(jnp.bfloat16)
        second.start()

    def finish(c, a):
        slot = lax.rem(c, 2)
        first, second = sums(c, a)
        done(residual(c, a))
        second.arrive()
        for b in range(2):
            at = slice(b * half, (b + 1) * half)
            wide = lambda ref: ref.astype(jnp.float32)
            total = keep_s[slot, a, 0, :, at] + wide(recv_s[slot, a, 1 - b, :, at]) + wide(recv_s[slot, a, 2, :, at])
            blk_s[slot, a, :, at] = (wide(res_s[slot, a, :, at]) + total).astype(jnp.bfloat16)
        first.leave()
        second.leave()

    for i in range(2):
        x_copy(0, i).start()
    go(w_copies(0))
    peers = [*ends[0], *ends[1], sibling]
    barrier = pltpu.get_barrier_semaphore()
    for k in peers:
        pl.semaphore_signal(barrier, inc=1, device_id=k, device_id_type=MESH)
    pl.semaphore_wait(barrier, len(peers))
    hop().start()
    near().start()

    def sum_end(c, a):
        finish(c, a)
        go(block_copies(c, a))

    def gather_one(c, a):
        done(block_copies(c, a))
        everywhere(c, a)[0].start()

    def gather_two(c, a):
        one, two, _, _ = everywhere(c, a)
        one.arrive()
        two.start()

    def gather_three(c, a):
        _, two, three, _ = everywhere(c, a)
        two.arrive()
        three.start()

    def gather_four(c, a):
        _, _, three, four = everywhere(c, a)
        three.arrive()
        four.start()

    def gather_end(c, a):
        all_ = everywhere(c, a)
        all_[3].arrive()
        for k in all_:
            k.leave()

    stages = dict(on=sum_on, end=sum_end, one=gather_one, two=gather_two, three=gather_three, four=gather_four, last=gather_end)

    def relay(p):
        first, second = ring(p - 1)
        first.arrive()
        second.start()

    def project_out(c, late, then, between=lambda: None):
        def before_0():
            late()
            go(o_copies(0, 1))

        product(c, 0, before_0, lambda: go(o_copies(1, 0)))
        between()
        product(c, 1, lambda: go(o_copies(1, 1)), then)
        for k in ring(c):
            k.leave()

    def period(p, _):
        def pick(at, other, pairs):
            for k, v in pairs:
                other = jnp.where(at == k, v, other)
            return other

        todo = []
        for lag in (3, 2, 1):
            for a in range(2):
                for name, times in zip(STAGES, TIMES[a]):
                    pairs = [(c, t % PLACES) for c, t in enumerate(times) if t // PLACES == c + 1 + lag]
                    if pairs:
                        todo.append((name, a, p - lag - 1, pick(p - lag - 1, -1, pairs), {v for _, v in pairs}))
        relay_at = pick(p, -1, enumerate(RELAYS, 1))

        def hooks(i):
            for name, a, c, when, places in todo:
                if (i in places) if isinstance(i, int) else any(1 <= k <= steps for k in places):
                    pl.when(when == i)(functools.partial(stages[name], c, a))

        def early(i, k, when, *todo):
            @pl.when((p == k) & (i == when))
            def _():
                for f in todo:
                    f()

        def inner(i):
            early(i, 0, 7, hop().arrive, on().start)
            early(i, 1, 5, near().arrive, near_swap.start)
            early(i, 1, 6, on().arrive, far_swap.start)
            early(i, 1, steps, near_swap.arrive)
            pl.when(relay_at == i)(lambda: relay(p))
            hooks(i)

        @pl.when(p > 1)
        def _():
            for a in range(2):
                go(residual(p - 2, a))

        hooks(0)
        norm(p)

        @pl.when(p + 1 < n)
        def _():
            for i in range(2):
                x_copy(p + 1, i).start()

        project(p, lambda i: inner(i + 1))

        hooks(steps + 1)
        attend(p)
        ring(p)[0].start()
        hooks(steps + 2)

        def next_period():
            pl.when(p + 1 < n)(lambda: go(w_copies(0)))

        pl.when(p == 0)(next_period)

        @pl.when(p > 0)
        def _():
            ring(p - 1)[1].arrive()
            project_out(p - 1, lambda: pl.when(p == 1)(far_swap.arrive), next_period, lambda: hooks(steps + 3))

        hooks(steps + 4)

    lax.fori_loop(0, n, period, None)
    go(o_copies(0, 0))
    for a in range(2):
        go(residual(n - 2, a))
    for name in TAIL:
        if name == "relay":
            relay(n)
        elif name == "product":
            ring(n - 1)[1].arrive()
            project_out(n - 1, lambda: None, lambda: None)
            for b in range(2):
                go(residual(n - 1, b))
        else:
            name, c, a = name.split()
            stages[name](int(c), int(a))
    for k in (hop(), on(), near(), near_swap, far_swap):
        k.leave()


STAGES = ("on", "end", "one", "two", "three", "four", "last")
PLACES = 13
TIMES = (
    (
        (27, 43, 56, 66, 80, 94),
        (30, 47, 60, 69, 85, 98),
        (31, 49, 61, 72, 87, 101),
        (35, 55, 66, 73, 93),
        (38, 57, 69, 81, 97),
        (46, 72, 76, 89),
        (50, 76, 87, 103),
    ),
    (
        (29, 41, 55, 70, 80, 95),
        (30, 47, 59, 73, 85, 99),
        (33, 48, 65, 74, 87, 102),
        (35, 51, 68, 76, 91),
        (38, 57, 73, 84, 97),
        (47, 67, 80, 90),
        (59, 75, 89, 97),
    ),
)
RELAYS = (8, 5, 5, 2, 2, 1, 8)
TAIL = (
    "relay", "four 4 1", "four 4 0", "two 5 0", "on 6 0", "on 6 1", "two 5 1", "product", "last 4 1", "last 4 0", "three 5 0",
    "end 6 0", "end 6 1", "one 6 0", "three 5 1", "one 6 1", "on 7 1", "on 7 0", "two 6 0", "four 5 0", "four 5 1", "two 6 1",
    "end 7 1", "end 7 0", "one 7 1", "three 6 0", "one 7 0", "last 5 0", "last 5 1", "three 6 1", "two 7 0", "two 7 1",
    "four 6 1", "four 6 0", "three 7 0", "three 7 1", "last 6 1", "last 6 0", "four 7 1", "four 7 0", "last 7 1", "last 7 0",
)


def layer(x, gain, wq, wk, wv, wo, tables, side):
    total, d = x.shape
    cols = wq.shape[1]
    r, n = CHUNK, total // CHUNK
    width = d // 2 // side
    rows = r // side
    vmem = lambda *s: pltpu.VMEM(s, jnp.bfloat16)
    wide = lambda *s: pltpu.VMEM(s, jnp.float32)
    dma = lambda *s: pltpu.SemaphoreType.DMA(s)
    whole = pl.BlockSpec(memory_space=pltpu.VMEM)
    blocks = _bf16(n, side, side, rows, width)
    return pl.pallas_call(
        functools.partial(_layer, side=side),
        in_specs=[ANY, whole, ANY, ANY, ANY, ANY] + [whole] * 4,
        out_specs=[ANY] * 4,
        out_shape=[blocks, blocks, _bf16(2, 2, side - 1, cols, width // 2), _bf16(2, 2, cols // 2, width // 2)],
        scratch_shapes=[
            vmem(2, PIECE, d), vmem(r, d), vmem(2, DEEP, 3 * cols), wide(r, 3 * cols),
            vmem(r, cols), vmem(total, cols), vmem(total, cols), wide(cols // HEAD, r), wide(cols // HEAD, HEAD + 8, r),
            vmem(3, 2, r, side * cols), wide(2, 2, 2, rows, width), vmem(2, 2, 3, rows, width), vmem(2, 2, 3, rows, width),
            vmem(2, 2, rows, width), vmem(2, 2, rows, width),
            dma(2), dma(2, 4), dma(2, 2), dma(2, 2), dma(2, 2), dma(2, 2), dma(2, 4), dma(2, 4), dma(2, 3), dma(2, 3),
            dma(3, 2, 4), dma(3, 2, 4), dma(2, 2, 4), dma(2, 2, 4), dma(4, 2, 8), dma(4, 2, 8),
        ],
        compiler_params=_params(collective_id=0, has_side_effects=True),
        cost_estimate=pl.CostEstimate(flops=8 * total * d * cols, transcendentals=0, bytes_accessed=8 * d * cols * n),
        name="layer",
    )(x, gain, wq, wk, wv, wo, *tables)


def _lay(g0_ref, g1_ref, y_ref, buf, in_sem, out_sem, *, side):
    n, _, _, rows, width = g0_ref.shape
    slots, units = buf.shape[0], 2 * n

    def on_part(u, f):
        for a in range(2):
            pl.when(lax.rem(u, 2) == a)(functools.partial(f, lax.div(u, 2), a, lax.rem(u, slots)))

    def ins(c, a, slot):
        return pltpu.make_async_copy((g0_ref, g1_ref)[a].at[c], buf.at[slot], in_sem.at[slot])

    def outs(c, a, slot):
        return [
            pltpu.make_async_copy(
                buf.at[slot, i, j],
                y_ref.at[pl.ds(pl.multiple_of((c * side + i) * rows, rows), rows), pl.ds((a * side + j) * width, width)],
                out_sem.at[slot, i, j],
            )
            for i in range(side) for j in range(side)
        ]

    def load(c, a, slot):
        ins(c, a, slot).start()

    def store(c, a, slot):
        ins(c, a, slot).wait()
        for k in outs(c, a, slot):
            k.start()

    def end(c, a, slot):
        for k in outs(c, a, slot):
            k.wait()

    ahead = slots // 2
    for u in range(ahead):
        on_part(jnp.int32(u), load)

    def one(u, _):
        pl.when(u >= slots - ahead)(lambda: on_part(u - slots + ahead, end))
        pl.when(u + ahead < units)(lambda: on_part(u + ahead, load))
        on_part(u, store)

    lax.fori_loop(0, units, one, None)
    for u in range(units - slots + ahead, units):
        on_part(jnp.int32(u), end)


def lay(g0, g1, shape, side):
    return pl.pallas_call(
        functools.partial(_lay, side=side),
        in_specs=[ANY, ANY],
        out_specs=ANY,
        out_shape=_bf16(*shape),
        scratch_shapes=[
            pltpu.VMEM((4, *g0.shape[1:]), jnp.bfloat16), pltpu.SemaphoreType.DMA((4,)), pltpu.SemaphoreType.DMA((4, side, side)),
        ],
        compiler_params=_params(),
        cost_estimate=pl.CostEstimate(flops=400 * g0.size, transcendentals=0, bytes_accessed=4 * (g0.size + g1.size)),
        name="lay",
    )(g0, g1)


def solution(mesh):
    side = math.isqrt(mesh.shape["tp"])

    def step(x, gain, wq, wk, wv, wo):
        rows = x.shape[0]

        def table(places):
            turn = np.float32(THETA) ** (-np.arange(HEAD // 2, dtype=np.float32) / np.float32(HEAD // 2))
            angle = places.astype(np.float32)[:, None] * turn
            cos, sin = np.cos(angle), np.sin(angle)
            return np.concatenate([cos, cos], 1), np.concatenate([-sin, sin], 1)

        tables = *table(np.arange(0, rows, CHUNK)), *table(np.arange(CHUNK))
        g0, g1, *_ = layer(x, gain[None], wq, wk, wv, wo, tables, side)
        return lay(g0, g1, x.shape, side)

    tokens, columns = P("dp", None), P(None, "tp")
    return jax.shard_map(
        step,
        mesh=mesh,
        in_specs=(tokens, P(None), columns, columns, columns, P("tp", None)),
        out_specs=tokens,
        check_vma=False,
    )
```
